32 devices in a mesh: front: 2 (over y), row: 4 (over x, core), col: 4 (over z).
Axes of the slice: x: 2, y: 2, z: 4, core: 2. Of those that a mesh axis runs over, the one named last changes fastest.
Arguments:
- front_cols: bfloat16 [16384, 256], P(('front', 'row'), 'col'), parts along dimension 0, as said below
- contrib: bfloat16 [8, 3072, 1536], P(('front', 'col'), 'row'), parts along dimension 0, as said below
- child_blocks: int32 [4, 24], P('front'), parts along dimension 0, may hold values from 0 to 63, as said below
- child_live: int32 [4], P('front'), parts along dimension 0, may hold values from 12 to 24
- finish: int32 [8], P('front'), parts along dimension 0, may hold values from 0 to 3, as said below
Outputs:
- schur: bfloat16 [16384, 8192], P(('front', 'row'), 'col'), parts along dimension 0
The draws below stay inside these ranges and needn't reach their ends.
There are 2 independent parts, one for each index of `front`. The reference program is written for one: setup_inputs(seed, part) draws one part's arguments, and reference() takes and returns one part's arrays. A program takes and returns all parts, laid end to end along the dimension named above; each array names one. Nothing has to cross between parts.
Inputs may be any that keep to these rules, and one draw needn't show every extreme that they name: `child_blocks`: row c holds distinct front blocks. With L the row sorted increasingly, entry q equals L[(q % 6) * 4 + 2 * (r % 2) + r // 2] where r = q // 6. At most 7 entries of a row lie in any aligned group of 16 consecutive block numbers, and exactly 7 in some group. `finish`: each value appears once. `contrib`: for each child c, the two pieces that finish names for c, left half then right half, form a symmetric positive definite matrix. `front_cols`: its leading 256 rows form a symmetric positive definite matrix.
All inputs are finite; a program needn't handle non-finite values.
Results may differ from the reference program's by a relative error of at most 0.008.
Values may be sent and summed in bfloat16 or wider, within the bound.
No kernel may reach another device: no remote copies, remote signals or barrier semaphores. Data moves between devices by JAX's collectives and lax.ppermute only.
A program may use at most 128 MiB of HBM per device.

```python
import jax
import jax.numpy as jnp
from jax import lax

NF = 8192
PANEL = 256
BLK = 128
MCB = 3072
SPREAD = 7
CHILDREN = 2
N_ROW = 4
N_COL = 4


def piece_order(key):
    return jax.random.permutation(jax.random.fold_in(key, 99), N_COL).astype(jnp.int32)


def draw_finish(key, part):
    return piece_order(key)


def draw_front_cols(key, part):
    basis_key, diagonal_key, couple_key = jax.random.split(key, 3)
    basis_matrix = jax.random.normal(basis_key, (PANEL, PANEL), jnp.float32)
    couple = 0.06 * jax.random.normal(couple_key, (NF - PANEL, PANEL), jnp.float32)
    diagonal = jax.random.uniform(diagonal_key, (PANEL,), jnp.float32, 0.5, 1.5)
    corner = jnp.dot(basis_matrix, basis_matrix.T, precision=lax.Precision.HIGHEST) / PANEL + jnp.diag(diagonal)
    return jnp.concatenate([corner, couple], axis=0).astype(jnp.bfloat16)


def draw_contrib(key, part):
    inner_width = MCB // 4
    half_width = MCB // 2

    def one_child(member):
        child_key = jax.random.fold_in(key, member)
        factor_key, diagonal_key = jax.random.split(child_key, 2)
        factor = jax.random.normal(factor_key, (MCB, inner_width), jnp.float32)
        diagonal = jax.random.uniform(diagonal_key, (MCB,), jnp.float32, 0.5, 1.5)
        gram = jnp.dot(factor, factor.T, precision=lax.Precision.HIGHEST) / inner_width + jnp.diag(diagonal)
        return gram.reshape(MCB, 2, half_width).transpose(1, 0, 2)
    blocks_all = jax.vmap(one_child)(jnp.arange(N_COL // 2, dtype=jnp.int32))
    pieces = blocks_all.reshape(N_COL, MCB, half_width)
    return pieces[piece_order(key)].astype(jnp.bfloat16)


def draw_child_blocks(key, part):
    group_count = N_ROW
    per_group = NF // (N_ROW * BLK)
    slot_count = group_count * SPREAD
    block_count = MCB // BLK
    run_length = MCB // (N_ROW * BLK)
    half_rows = N_ROW // 2
    places = jnp.arange(block_count, dtype=jnp.int32)
    device_row = places // run_length
    residue = 2 * (device_row % half_rows) + device_row // half_rows
    source_place = places % run_length * N_ROW + residue

    def one_child(member):
        child_key = jax.random.fold_in(key, member + 7)
        pick_key, order_key, offset_key = jax.random.split(child_key, 3)
        favoured = jax.random.randint(pick_key, (), 0, group_count)
        ranking = jax.random.permutation(order_key, slot_count).astype(jnp.int32)
        slot_ids = jnp.arange(slot_count, dtype=jnp.int32)
        scores = ranking + jnp.where(slot_ids // SPREAD == favoured, -slot_count, 0)
        chosen = jnp.argsort(scores, stable=True)[:block_count].astype(jnp.int32)

        def group_offsets(group_key):
            return jnp.sort(jax.random.permutation(group_key, per_group)[:SPREAD].astype(jnp.int32))
        offsets = jax.vmap(group_offsets)(jax.random.split(offset_key, group_count))
        parent = chosen // SPREAD * per_group + offsets[chosen // SPREAD, chosen % SPREAD]
        ordered = jnp.sort(parent).astype(jnp.int32)
        return ordered[source_place].astype(jnp.int32)
    return jax.vmap(one_child)(jnp.arange(N_COL // 2, dtype=jnp.int32))


def setup_inputs(seed: int = 0, part: int = 0) -> dict:
    splits = jax.random.split(jax.random.key(seed), 6)
    own_keys = jax.random.split(jax.random.fold_in(splits[5], part), 6)
    front_cols = draw_front_cols(jax.random.fold_in(jax.random.fold_in(splits[5], part), 71), part)
    contrib = draw_contrib(jax.random.fold_in(jax.random.fold_in(splits[5], part), 71), part)
    child_blocks = draw_child_blocks(jax.random.fold_in(jax.random.fold_in(splits[5], part), 71), part)
    child_live = jax.random.randint(own_keys[3], (CHILDREN,), MCB // (2 * BLK), MCB // BLK + 1).astype(jnp.int32)
    finish = draw_finish(jax.random.fold_in(jax.random.fold_in(splits[5], part), 71), part)
    return dict(front_cols=front_cols, contrib=contrib, child_blocks=child_blocks, child_live=child_live, finish=finish)


def reference(front_cols, contrib, child_blocks, child_live, finish):
    offsets = jnp.arange(BLK, dtype=jnp.int32)
    lane_ids = jnp.arange(MCB, dtype=jnp.int32)
    piece_ids = jnp.arange(N_COL, dtype=jnp.int32)
    order = finish.astype(jnp.int32)
    assembled = jnp.zeros((NF, NF), jnp.float32)
    assembled = assembled.at[:, :PANEL].add(front_cols.astype(jnp.float32))
    for child in range(N_COL // 2):
        left_at = jnp.sum(jnp.where(order == 2 * child, piece_ids, 0)).astype(jnp.int32)
        right_at = jnp.sum(jnp.where(order == 2 * child + 1, piece_ids, 0)).astype(jnp.int32)
        contribution = jnp.concatenate([contrib[left_at], contrib[right_at]], axis=1).astype(jnp.float32)
        live_rows = child_live[child].astype(jnp.int32) * BLK
        keep_mask = (lane_ids[:, None] < live_rows) & (lane_ids[None, :] < live_rows) & (lane_ids[:, None] >= lane_ids[None, :])
        contribution = jnp.where(keep_mask, contribution, 0.0)
        position = (child_blocks[child].astype(jnp.int32)[:, None] * BLK + offsets[None, :]).reshape(-1)
        assembled = assembled.at[position[:, None], position[None, :]].add(contribution)
    row_ids = jnp.arange(NF, dtype=jnp.int32)
    lower_part = row_ids[:, None] >= row_ids[None, :]
    assembled = jnp.where(lower_part, assembled, 0.0)
    corner = assembled[:PANEL, :PANEL]
    corner = corner + jnp.tril(corner, -1).T
    factor = jnp.linalg.cholesky(corner)
    solved = lax.linalg.triangular_solve(factor, assembled[:, :PANEL], left_side=False, lower=True, transpose_a=True)
    update = jnp.dot(solved.astype(jnp.float32), solved.T.astype(jnp.float32), precision=lax.Precision.HIGHEST, preferred_element_type=jnp.float32)
    keep_out = lower_part & (row_ids[:, None] >= PANEL) & (row_ids[None, :] >= PANEL)
    return jnp.where(keep_out, assembled - update, 0.0).astype(jnp.bfloat16)
```

```python
import functools

import jax
import jax.numpy as jnp
from jax import lax
from jax.experimental import pallas as pl
from jax.experimental.pallas import tpu as pltpu
from jax.sharding import PartitionSpec as P

PANEL = 256
BLK = 128
PB = PANEL // BLK
F32 = jnp.float32
BF16 = jnp.bfloat16


class Plan:
    def __init__(self, nr, nc, local, piece_rows, piece_cols, children):
        self.nr, self.nc, self.local = nr, nc, local
        self.group = local // BLK
        self.rb = piece_rows // BLK
        self.cb = piece_cols // BLK
        self.hr = nr // 2
        self.children = children
        self.cw = PANEL // nc
        spread = self.rb + 1
        self.rk = -(-spread // nr)
        self.split = self.rk * (-(-self.rk // 2))
        same = self.rk * self.rk + (self.hr - 1) * self.split
        cross = self.rk * self.rk * (-(-self.hr // 2))
        self.slots = max(same, cross)
        self.pan = self.hr * self.rk

    def res(self, r):
        return 2 * (r % self.hr) + r // self.hr

    def decode(self, s, r, h):
        rk, hr = self.rk, self.hr
        half, ri = r // hr, r % hr
        if s < rk * rk:
            same = (ri, s // rk, s % rk)
        else:
            t = s - rk * rk
            i, w = t // self.split, t % self.split
            oi = i + jnp.where(i >= ri, 1, 0)
            flip = jnp.where(oi > ri, 1, 0)
            parity = (ri + oi + flip) % 2
            same = (oi, 2 * (w // rk) + parity, w % rk)
        i, w = s // (rk * rk), s % (rk * rk)
        oi = 2 * i + (r + h) % 2
        cross = (oi, w // rk, w % rk)
        is_same = half == h
        oi = jnp.where(is_same, same[0], cross[0])
        rank_a = jnp.where(is_same, same[1], cross[1])
        rank_b = jnp.where(is_same, same[2], cross[2])
        o = h * hr + oi
        ok = (oi < hr) & (rank_a < rk)
        return o, o > r, rank_a, rank_b, ok

    def first(self, kf, c, cls, g):
        return kf[(c * self.nr + cls) * (self.nr + 1) + g]


def pack_kernel(plan, pos, kf, finish, piece, front, *rest):
    nr, nc, rb = plan.nr, plan.nc, plan.rb
    flows = nr * nc
    bulk = rest[:flows]
    pan = rest[flows:flows + nr]
    corner, ft, sems, psems, csem = rest[flows + nr:]
    r, z = pos[0], pos[1]
    piece_id = finish[z]
    c, h = piece_id // 2, piece_id % 2

    def block(row, col):
        row = pl.multiple_of(row * BLK, BLK)
        col = pl.multiple_of(col * BLK, BLK)
        return piece.at[pl.ds(row, BLK), pl.ds(col, BLK)]

    corner_copy = pltpu.make_async_copy(block(0, 0), corner.at[pl.ds(0, BLK), :], csem)
    corner_copy.start()

    def pan_copies(dr):
        g = (r + dr) % nr
        for s in range(plan.pan):
            oi, rank = s // plan.rk, s % plan.rk
            k = plan.first(kf, c, h * plan.hr + oi, g) + rank
            col = oi * rb + jnp.minimum(k, rb - 1)
            yield pltpu.make_async_copy(block(0, col), pan[dr].at[s], psems.at[dr * plan.pan + s])

    sends_pan = (r % plan.hr) == 0

    @pl.when(sends_pan)
    def _():
        for dr in range(nr):
            for copy in pan_copies(dr):
                copy.start()

    slots = [plan.decode(s, r, h) for s in range(plan.slots)]

    def flow_copies(k):
        dest_r = (r + k // nc) % nr
        dest_c = (z + k % nc) % nc
        for s, (o, flip, rank_a, rank_b, ok) in enumerate(slots):
            row_group = jnp.where(flip, dest_c, dest_r)
            col_group = jnp.where(flip, dest_r, dest_c)
            row = plan.first(kf, c, r, row_group) + jnp.where(flip, rank_b, rank_a)
            oc = jnp.minimum(o, nr - 1)
            col = plan.first(kf, c, oc, col_group) + jnp.where(flip, rank_a, rank_b)
            row = jnp.minimum(row, rb - 1)
            col = (oc - h * plan.hr) * rb + jnp.minimum(col, rb - 1)
            col = jnp.clip(col, 0, plan.cb - 1)
            yield pltpu.make_async_copy(block(row, col), bulk[k].at[s], sems.at[k * plan.slots + s])

    for k in range(flows):
        @pl.when((r + k // nc) % nr >= (z + k % nc) % nc)
        def _(k=k):
            for copy in flow_copies(k):
                copy.start()

    turned = jnp.transpose(front[...].astype(F32)).astype(BF16)
    ft[...] = turned
    for t in range(PB):
        corner[pl.ds(BLK + t * plan.cw, plan.cw), :] = turned[:, t * BLK:(t + 1) * BLK]
    corner_copy.wait()

    @pl.when(sends_pan)
    def _():
        for dr in range(nr):
            for s in range(plan.pan):
                pltpu.make_async_copy(block(0, 0), pan[dr].at[s], psems.at[dr * plan.pan + s]).wait()

    for k in range(flows):
        @pl.when((r + k // nc) % nr >= (z + k % nc) % nc)
        def _(k=k):
            for s in range(plan.slots):
                pltpu.make_async_copy(block(0, 0), bulk[k].at[s], sems.at[k * plan.slots + s]).wait()


def three_parts(x):
    hi = x.astype(BF16)
    rest = x - hi.astype(F32)
    mid = rest.astype(BF16)
    low = (rest - mid.astype(F32)).astype(BF16)
    return hi, mid, low


def factor_rows(w, size):
    lanes, step, width = 128, 8, 32
    ktiles = size // lanes

    for top in range(0, size, width):
        for b in range(top, top + width, step):
            kt, off = b // lanes, b % lanes
            tiles = list(range(kt, ktiles)) + [ktiles + t for t in range(kt + 1)]

            def load(i):
                return {t: w[pl.ds(i, 1), t * lanes:(t + 1) * lanes] for t in tiles}

            rows = [load(b + i) for i in range(step)]
            d = {}
            for i in range(step):
                for j in range(i, step):
                    d[i, j] = jnp.broadcast_to(rows[i][kt][:, off + j:off + j + 1], (1, lanes))
            for i in range(step):
                inv = lax.rsqrt(d[i, i])
                u = {j: d[i, j] * inv for j in range(i + 1, step)}
                for t in tiles:
                    rows[i][t] = rows[i][t] * inv
                for j in range(i + 1, step):
                    for m in range(j, step):
                        d[j, m] = d[j, m] - u[j] * u[m]
                    for t in tiles:
                        rows[j][t] = rows[j][t] - u[j] * rows[i][t]
            for i in range(step):
                for t in tiles:
                    w[pl.ds(b + i, 1), t * lanes:(t + 1) * lanes] = rows[i][t]
            for n in range(b + step, top + width):
                below = load(n)
                at = n % lanes
                for i in range(step):
                    u = jnp.broadcast_to(rows[i][n // lanes][:, at:at + 1], (1, lanes))
                    for t in tiles:
                        below[t] = below[t] - u * rows[i][t]
                for t in tiles:
                    w[pl.ds(n, 1), t * lanes:(t + 1) * lanes] = below[t]
        low = top + width
        if low < size:
            full = w[pl.ds(top, width), :]
            base = (low // lanes) * lanes
            left = jnp.transpose(w[pl.ds(top, width), base:size])[low - base:, :]
            a, b2, c2 = three_parts(left)
            x, y, v = three_parts(full)
            lhs = jnp.concatenate([a, a, b2, b2, a, c2], axis=1)
            rhs = jnp.concatenate([x, y, x, y, v, x], axis=0)
            w[pl.ds(low, size - low), :] = w[pl.ds(low, size - low), :] - jnp.dot(
                lhs, rhs, preferred_element_type=F32)


def solve_kernel(plan, pos, kf, blocks, live, finish, st0, st1, *rest):
    nr, nc, rb, hr, cw = plan.nr, plan.nc, plan.rb, plan.hr, plan.cw
    fts, pans = rest[:nc], rest[nc:2 * nc]
    rp, cpt, w, at = rest[2 * nc:]
    r, z = pos[0], pos[1]
    nb = rb * nr

    @pl.when(r >= z)
    def _():
        eye_r = lax.broadcasted_iota(jnp.int32, (PANEL, PANEL), 0)
        eye_c = lax.broadcasted_iota(jnp.int32, (PANEL, PANEL), 1)
        w[:, PANEL:] = jnp.where(eye_r == eye_c, 1.0, 0.0).astype(F32)
        for dz in range(nc):
            src = (z + nc - dz) % nc
            k0 = pl.multiple_of(src * cw, cw)
            for t in range(PB):
                w[pl.ds(k0, cw), t * BLK:(t + 1) * BLK] = st0[dz, pl.ds(BLK + t * cw, cw), :].astype(F32)
        for dz in range(nc):
            piece_id = finish[(z + nc - dz) % nc]
            c, h = piece_id // 2, piece_id % 2
            b0 = blocks[c * nb]
            b1 = blocks[c * nb + plan.cb]
            second = (b1 < PB) & (plan.cb < live[c])

            def add(row, col, value):
                rs = pl.ds(pl.multiple_of(row * BLK, BLK), BLK)
                cs = pl.ds(pl.multiple_of(col * BLK, BLK), BLK)
                w[rs, cs] = w[rs, cs] + value.astype(F32)

            @pl.when((h == 0) & (b0 < PB))
            def _():
                add(b0, b0, st0[dz, pl.ds(0, BLK), :])

            @pl.when((h == 1) & second)
            def _():
                add(b0, b1, st0[dz, pl.ds(0, BLK), :])
                add(b1, b1, st1[dz, pl.ds(0, BLK), :])

        factor_rows(w, PANEL)

        for dz in range(nc):
            src = (z + nc - dz) % nc
            at[pl.ds(pl.multiple_of(src * cw, cw), cw), :] = fts[dz][...].astype(F32)
        for dz in range(nc):
            piece_id = finish[(z + nc - dz) % nc]
            c, h = piece_id // 2, piece_id % 2
            for which in range(2):
                qb = which * plan.cb
                fb = blocks[c * nb + qb]
                use = fb < PB
                if which:
                    use = use & (h == 1) & (qb < live[c])

                @pl.when(use)
                def _(which=which, fb=fb, dz=dz, c=c, h=h):
                    for s in range(plan.pan):
                        oi, rank = s // plan.rk, s % plan.rk
                        o = h * hr + oi
                        k = plan.first(kf, c, o, r) + rank
                        qa = jnp.minimum(o * rb + k, nb - 1)

                        @pl.when((k < plan.first(kf, c, o, r + 1)) & (qa < live[c]))
                        def _():
                            gi = blocks[c * nb + qa] % plan.group
                            rs = pl.ds(pl.multiple_of(fb * BLK, BLK), BLK)
                            cs = pl.ds(pl.multiple_of(gi * BLK, BLK), BLK)
                            at[rs, cs] = at[rs, cs] + pans[dz][which, s].astype(F32)

        inv = w[:, PANEL:]
        inv_hi = inv.astype(BF16)
        inv_lo = (inv - inv_hi.astype(F32)).astype(BF16)

        def solve(i, carry):
            cs = pl.ds(pl.multiple_of(i * 256, 256), 256)
            a = at[:, cs]
            a_hi = a.astype(BF16)
            a_lo = (a - a_hi.astype(F32)).astype(BF16)
            p = jnp.dot(inv_hi, a_hi, preferred_element_type=F32)
            p = p + jnp.dot(inv_hi, a_lo, preferred_element_type=F32)
            p = p + jnp.dot(inv_lo, a_hi, preferred_element_type=F32)
            cpt[:, cs] = p.astype(BF16)
            rp[cs, :] = (-jnp.transpose(p)).astype(BF16)
            return carry

        lax.fori_loop(0, plan.local // 256, solve, 0)


def final_kernel(plan, pos, kf, blocks, live, finish, rp, *rest):
    nr, nc, rb = plan.nr, plan.nc, plan.rb
    flows = nr * nc
    cpts, bulk = rest[:nr], rest[nr:nr + flows]
    out, rpv, cpv, inbox, acc, stage, in_sems, out_sems = rest[nr + flows:]
    r, z = pos[0], pos[1]
    nb = rb * nr
    strip = 128
    strips = plan.local // strip

    def out_copy(i, slot):
        rows = pl.ds(pl.multiple_of(i * strip, strip), strip)
        return pltpu.make_async_copy(stage.at[slot], out.at[rows, :], out_sems.at[slot])

    @pl.when(r < z)
    def _():
        stage[0] = jnp.zeros_like(stage[0])
        stage[1] = jnp.zeros_like(stage[1])

        def body(i, carry):
            @pl.when(i >= 2)
            def _():
                out_copy(i, i % 2).wait()
            out_copy(i, i % 2).start()
            return carry

        lax.fori_loop(0, strips, body, 0)
        out_copy(0, 0).wait()
        out_copy(1, 1).wait()

    @pl.when(r >= z)
    def _():
        rp_copy = pltpu.make_async_copy(rp, rpv, in_sems.at[0])
        rp_copy.start()
        for dr in range(nr):
            @pl.when(r - z == dr)
            def _(dr=dr):
                pltpu.make_async_copy(cpts[dr], cpv, in_sems.at[1]).start()

        def bulk_copy(k):
            return pltpu.make_async_copy(
                bulk[k], inbox.at[pl.ds(k * plan.slots, plan.slots)], in_sems.at[2 + k])

        for k in range(flows):
            bulk_copy(k).start()
        rp_copy.wait()
        pltpu.make_async_copy(cpts[0], cpv, in_sems.at[1]).wait()

        def multiply(i, carry):
            rows = pl.ds(pl.multiple_of(i * 256, 256), 256)
            acc[rows, :] = jnp.dot(rpv[rows, :], cpv[...], preferred_element_type=F32)
            return carry

        lax.fori_loop(0, plan.local // 256, multiply, 0)

        for k in range(flows):
            bulk_copy(k).wait()
            src_r = (r + nr - k // nc) % nr
            src_z = (z + nc - k % nc) % nc
            piece_id = finish[src_z]
            c, h = piece_id // 2, piece_id % 2
            for s in range(plan.slots):
                o, flip, rank_a, rank_b, ok = plan.decode(s, src_r, h)
                o = jnp.minimum(o, nr - 1)
                ra = jnp.where(flip, o, src_r)
                rb_ = jnp.where(flip, src_r, o)
                ka = plan.first(kf, c, ra, r) + rank_a
                kb = plan.first(kf, c, rb_, z) + rank_b
                ok = ok & (ka < plan.first(kf, c, ra, r + 1)) & (kb < plan.first(kf, c, rb_, z + 1))
                qa = ra * rb + ka
                qb = rb_ * rb + kb
                pa = ka * nr + plan.res(ra)
                pb = kb * nr + plan.res(rb_)
                ok = ok & (pa >= pb) & (qa >= qb) & (qa < live[c])
                gi = blocks[c * nb + jnp.clip(qa, 0, nb - 1)] % plan.group
                gj = blocks[c * nb + jnp.clip(qb, 0, nb - 1)] % plan.group
                rs = pl.ds(pl.multiple_of(gi * BLK, BLK), BLK)
                cs = pl.ds(pl.multiple_of(gj * BLK, BLK), BLK)

                @pl.when(ok & jnp.logical_not(flip))
                def _():
                    acc[rs, cs] = acc[rs, cs] + inbox[k * plan.slots + s].astype(F32)

                @pl.when(ok & flip)
                def _():
                    acc[rs, cs] = acc[rs, cs] + jnp.transpose(inbox[k * plan.slots + s].astype(F32))

        def finish_strip(i, carry):
            slot = i % 2

            @pl.when(i >= 2)
            def _():
                out_copy(i, slot).wait()
            rows = pl.ds(pl.multiple_of(i * strip, strip), strip)
            row_ids = r * plan.local + i * strip + lax.broadcasted_iota(jnp.int32, (strip, plan.local), 0)
            col_ids = z * plan.local + lax.broadcasted_iota(jnp.int32, (strip, plan.local), 1)
            keep = (row_ids >= col_ids) & (col_ids >= PANEL)
            stage[slot] = jnp.where(keep, acc[rows, :], 0.0).astype(BF16)
            out_copy(i, slot).start()
            return carry

        lax.fori_loop(0, strips, finish_strip, 0)
        out_copy(0, 0).wait()
        out_copy(1, 1).wait()


def body(front_cols, contrib, child_blocks, child_live, finish):
    nr, nc = lax.axis_size("row"), lax.axis_size("col")
    own_row, own_col = lax.axis_index("row"), lax.axis_index("col")
    local = front_cols.shape[0]
    piece = contrib[0]
    children = child_blocks.shape[0]
    plan = Plan(nr, nc, local, piece.shape[0], piece.shape[1], children)
    flows = nr * nc
    both = ("row", "col")

    pos = jnp.stack([own_row, own_col]).astype(jnp.int32)
    owner = child_blocks.reshape(children, nr, plan.rb, 1) // plan.group
    kf = jnp.sum(owner < jnp.arange(nr + 1, dtype=jnp.int32), axis=2, dtype=jnp.int32).reshape(-1)
    blocks = child_blocks.reshape(-1)

    def pairs(dr, dz, wanted):
        found = []
        for r in range(nr):
            for z in range(nc):
                to_r, to_c = (r + dr) % nr, (z + dz) % nc
                if wanted(r, z, to_r, to_c):
                    found.append((r * nc + z, to_r * nc + to_c))
        return found

    def send(x, dr, dz, wanted):
        return lax.ppermute(x, both, pairs(dr, dz, wanted))

    smem = pl.BlockSpec(memory_space=pltpu.SMEM)
    vmem = pl.BlockSpec(memory_space=pltpu.VMEM)
    anyw = pl.BlockSpec(memory_space=pl.ANY)
    slot_shape = (plan.slots, BLK, BLK)
    corner_shape = (BLK + PB * plan.cw, BLK)

    packed = pl.pallas_call(
        functools.partial(pack_kernel, plan),
        name="pack",
        in_specs=[smem, smem, smem, anyw, vmem],
        out_specs=[anyw] * (flows + nr) + [vmem, vmem],
        out_shape=[jax.ShapeDtypeStruct(slot_shape, BF16)] * flows
        + [jax.ShapeDtypeStruct((plan.pan, BLK, BLK), BF16)] * nr
        + [jax.ShapeDtypeStruct(corner_shape, BF16), jax.ShapeDtypeStruct((plan.cw, local), BF16)],
        scratch_shapes=[
            pltpu.SemaphoreType.DMA((flows * plan.slots,)),
            pltpu.SemaphoreType.DMA((nr * plan.pan,)),
            pltpu.SemaphoreType.DMA,
        ],
    )(pos, kf, finish, piece, front_cols)
    bulk, pan = packed[:flows], packed[flows:flows + nr]
    corner, ft = packed[flows + nr:]

    source_row = lambda r, z, R, C: r % plan.hr == 0
    lower = lambda r, z, R, C: R >= C

    corners = [corner] + [send(corner, 0, dz, source_row) for dz in range(1, nc)]
    corners = jnp.stack(corners)
    stacks = [corners] + [send(corners, dr, 0, source_row) for dr in range(1, nr)]
    pans = [pan[0]] + [send(pan[dr], dr, 0, source_row) for dr in range(1, nr)]

    def from_row(values, row):
        shift = (own_row - row) % nr
        got = values[0]
        for dr in range(1, nr):
            got = jnp.where(shift == dr, values[dr], got)
        return got

    st0, st1 = from_row(stacks, 0), from_row(stacks, plan.hr)
    pan_own = jnp.stack([from_row(pans, 0), from_row(pans, plan.hr)])
    fts = [ft] + [send(ft, 0, dz, lower) for dz in range(1, nc)]
    pan_all = [pan_own] + [send(pan_own, 0, dz, lower) for dz in range(1, nc)]

    rp, cpt = pl.pallas_call(
        functools.partial(solve_kernel, plan),
        name="solve",
        in_specs=[smem] * 5 + [vmem] * (2 + 2 * nc),
        out_specs=[vmem, vmem],
        out_shape=[jax.ShapeDtypeStruct((local, PANEL), BF16), jax.ShapeDtypeStruct((PANEL, local), BF16)],
        scratch_shapes=[pltpu.VMEM((PANEL, 2 * PANEL), F32), pltpu.VMEM((PANEL, local), F32)],
    )(pos, kf, blocks, child_live, finish, st0, st1, *fts, *pan_all)

    cpts = [cpt] + [send(cpt, dr, 0, lambda r, z, R, C: r == z and R > r) for dr in range(1, nr)]
    received = [bulk[0]] + [send(bulk[k], k // nc, k % nc, lower) for k in range(1, flows)]

    return pl.pallas_call(
        functools.partial(final_kernel, plan),
        name="final",
        in_specs=[smem] * 5 + [anyw] * (1 + nr + flows),
        out_specs=anyw,
        out_shape=jax.ShapeDtypeStruct((local, local), BF16),
        scratch_shapes=[
            pltpu.VMEM((local, PANEL), BF16),
            pltpu.VMEM((PANEL, local), BF16),
            pltpu.VMEM((flows * plan.slots, BLK, BLK), BF16),
            pltpu.VMEM((local, local), F32),
            pltpu.VMEM((2, 128, local), BF16),
            pltpu.SemaphoreType.DMA((2 + flows,)),
            pltpu.SemaphoreType.DMA((2,)),
        ],
    )(pos, kf, blocks, child_live, finish, rp, *cpts, *received)


def solution(mesh):
    return jax.shard_map(
        body,
        mesh=mesh,
        in_specs=(
            P(("front", "row"), "col"),
            P(("front", "col"), "row", None),
            P("front", None),
            P("front"),
            P("front"),
        ),
        out_specs=P(("front", "row"), "col"),
        check_vma=False,
    )
```

```python
import functools

import jax
import jax.numpy as jnp
from jax import lax
from jax.experimental import pallas as pl
from jax.experimental.pallas import tpu as pltpu
from jax.sharding import PartitionSpec as P


PANEL = 256
BLK = 128
PB = PANEL // BLK
F32 = jnp.float32
BF16 = jnp.bfloat16


class Plan:
    def __init__(self, nr, nc, local, piece_rows, piece_cols, children):
        self.nr, self.nc, self.local = nr, nc, local
        self.group = local // BLK
        self.rb = piece_rows // BLK
        self.cb = piece_cols // BLK
        self.hr = nr // 2
        self.children = children
        self.cw = PANEL // nc
        spread = self.rb + 1
        self.rk = -(-spread // nr)
        self.split = self.rk * (-(-self.rk // 2))
        same = self.rk * self.rk + (self.hr - 1) * self.split
        cross = self.rk * self.rk * (-(-self.hr // 2))
        self.slots = max(same, cross)
        self.pan = self.hr * self.rk

    def res(self, r):
        return 2 * (r % self.hr) + r // self.hr

    def decode(self, s, r, h):
        rk, hr = self.rk, self.hr
        half, ri = r // hr, r % hr
        if s < rk * rk:
            same = (ri, s // rk, s % rk)
        else:
            t = s - rk * rk
            i, w = t // self.split, t % self.split
            oi = i + jnp.where(i >= ri, 1, 0)
            flip = jnp.where(oi > ri, 1, 0)
            parity = (ri + oi + flip) % 2
            same = (oi, 2 * (w // rk) + parity, w % rk)
        i, w = s // (rk * rk), s % (rk * rk)
        oi = 2 * i + (r + h) % 2
        cross = (oi, w // rk, w % rk)
        is_same = half == h
        oi = jnp.where(is_same, same[0], cross[0])
        rank_a = jnp.where(is_same, same[1], cross[1])
        rank_b = jnp.where(is_same, same[2], cross[2])
        o = h * hr + oi
        ok = (oi < hr) & (rank_a < rk)
        return o, o > r, rank_a, rank_b, ok

    def fill(self, kf, blocks, child):
        for cls in range(self.nr):
            at = [blocks[child, cls * self.rb + k] for k in range(self.rb)]
            for g in range(self.nr + 1):
                count = 0
                for b in at:
                    count = count + jnp.where(b < g * self.group, 1, 0)
                kf[(child * self.nr + cls) * (self.nr + 1) + g] = count

    def first(self, kf, c, cls, g):
        return kf[(c * self.nr + cls) * (self.nr + 1) + g]

    def table(self):
        return pltpu.SMEM((self.children * self.nr * (self.nr + 1),), jnp.int32)


def pack_kernel(plan, blocks, finish, piece, front, *rest):
    nr, nc, rb = plan.nr, plan.nc, plan.rb
    flows = nr * nc
    bulk = rest[:flows]
    pan = rest[flows:flows + nr]
    corner, kf = rest[flows + nr:]
    r, z = lax.axis_index("row"), lax.axis_index("col")
    piece_id = finish[z]
    c, h = piece_id // 2, piece_id % 2
    plan.fill(kf, blocks, c)

    def block(row, col):
        row = pl.multiple_of(row * BLK, BLK)
        col = pl.multiple_of(col * BLK, BLK)
        return piece[0, pl.ds(row, BLK), pl.ds(col, BLK)]

    @pl.when((r % plan.hr) == 0)
    def _():
        corner[:BLK, :] = block(0, 0)
        for t in range(PB):
            corner[BLK + t * plan.cw:BLK + (t + 1) * plan.cw, :] = front[:, t * BLK:(t + 1) * BLK]
        for dr in range(nr):
            g = (r + dr) % nr
            for s in range(plan.pan):
                oi, rank = s // plan.rk, s % plan.rk
                k = plan.first(kf, c, h * plan.hr + oi, g) + rank
                pan[dr][s] = block(0, oi * rb + jnp.minimum(k, rb - 1))

    slots = [plan.decode(s, r, h) for s in range(plan.slots)]
    for k in range(flows):
        dest_r = (r + k // nc) % nr
        dest_c = (z + k % nc) % nc

        @pl.when(dest_r >= dest_c)
        def _(k=k, dest_r=dest_r, dest_c=dest_c):
            for s, (o, flip, rank_a, rank_b, ok) in enumerate(slots):
                row_group = jnp.where(flip, dest_c, dest_r)
                col_group = jnp.where(flip, dest_r, dest_c)
                row = plan.first(kf, c, r, row_group) + jnp.where(flip, rank_b, rank_a)
                oc = jnp.minimum(o, nr - 1)
                col = plan.first(kf, c, oc, col_group) + jnp.where(flip, rank_a, rank_b)
                row = jnp.minimum(row, rb - 1)
                col = (oc - h * plan.hr) * rb + jnp.minimum(col, rb - 1)
                bulk[k][s] = block(row, jnp.clip(col, 0, plan.cb - 1))


def three_parts(x):
    hi = x.astype(BF16)
    rest = x - hi.astype(F32)
    mid = rest.astype(BF16)
    low = (rest - mid.astype(F32)).astype(BF16)
    return hi, mid, low


def factor_rows(w, size):
    lanes, step, width = 128, 8, 32
    ktiles = size // lanes

    for top in range(0, size, width):
        for b in range(top, top + width, step):
            kt, off = b // lanes, b % lanes
            tiles = list(range(kt, ktiles)) + [ktiles + t for t in range(kt + 1)]

            def load(i):
                return {t: w[pl.ds(i, 1), t * lanes:(t + 1) * lanes] for t in tiles}

            rows = [load(b + i) for i in range(step)]
            d = {}
            for i in range(step):
                for j in range(i, step):
                    d[i, j] = jnp.broadcast_to(rows[i][kt][:, off + j:off + j + 1], (1, lanes))
            for i in range(step):
                inv = lax.rsqrt(d[i, i])
                u = {j: d[i, j] * inv for j in range(i + 1, step)}
                for t in tiles:
                    rows[i][t] = rows[i][t] * inv
                for j in range(i + 1, step):
                    for m in range(j, step):
                        d[j, m] = d[j, m] - u[j] * u[m]
                    for t in tiles:
                        rows[j][t] = rows[j][t] - u[j] * rows[i][t]
            for i in range(step):
                for t in tiles:
                    w[pl.ds(b + i, 1), t * lanes:(t + 1) * lanes] = rows[i][t]
            for n in range(b + step, top + width):
                below = load(n)
                at = n % lanes
                for i in range(step):
                    u = jnp.broadcast_to(rows[i][n // lanes][:, at:at + 1], (1, lanes))
                    for t in tiles:
                        below[t] = below[t] - u * rows[i][t]
                for t in tiles:
                    w[pl.ds(n, 1), t * lanes:(t + 1) * lanes] = below[t]
        low = top + width
        if low < size:
            full = w[pl.ds(top, width), :]
            base = (low // lanes) * lanes
            left = jnp.transpose(w[pl.ds(top, width), base:size])[low - base:, :]
            a, b2, c2 = three_parts(left)
            x, y, v = three_parts(full)
            lhs = jnp.concatenate([a, a, b2, b2, a, c2], axis=1)
            rhs = jnp.concatenate([x, y, x, y, v, x], axis=0)
            w[pl.ds(low, size - low), :] = w[pl.ds(low, size - low), :] - jnp.dot(
                lhs, rhs, preferred_element_type=F32)


def factor_kernel(plan, blocks, live, finish, *rest):
    nr, nc, cw = plan.nr, plan.nc, plan.cw
    stacks, inv_out, w = rest[:nr], rest[nr], rest[nr + 1]
    r, z = lax.axis_index("row"), lax.axis_index("col")
    height = BLK + PB * cw

    def add(row, col, value):
        rs = pl.ds(pl.multiple_of(row * BLK, BLK), BLK)
        cs = pl.ds(pl.multiple_of(col * BLK, BLK), BLK)
        w[rs, cs] = w[rs, cs] + value.astype(F32)

    def child(dz):
        piece_id = finish[(z + nc - dz) % nc]
        c, h = piece_id // 2, piece_id % 2
        b0, b1 = blocks[c, 0], blocks[c, plan.cb]
        return h, b0, b1, (b1 < PB) & (plan.cb < live[c])

    def from_first(stack):
        for dz in range(nc):
            k0 = pl.multiple_of((z + nc - dz) % nc * cw, cw)
            for t in range(PB):
                at = dz * height + BLK + t * cw
                w[pl.ds(k0, cw), t * BLK:(t + 1) * BLK] = stack[at:at + cw, :].astype(F32)
        for dz in range(nc):
            h, b0, b1, second = child(dz)

            @pl.when((h == 0) & (b0 < PB))
            def _():
                add(b0, b0, stack[dz * height:dz * height + BLK, :])

            @pl.when((h == 1) & second)
            def _():
                add(b0, b1, stack[dz * height:dz * height + BLK, :])

    def from_second(stack):
        for dz in range(nc):
            h, _, b1, second = child(dz)

            @pl.when((h == 1) & second)
            def _():
                add(b1, b1, stack[dz * height:dz * height + BLK, :])

    @pl.when(r >= z)
    def _():
        eye_r = lax.broadcasted_iota(jnp.int32, (PANEL, PANEL), 0)
        eye_c = lax.broadcasted_iota(jnp.int32, (PANEL, PANEL), 1)
        w[:, PANEL:] = jnp.where(eye_r == eye_c, 1.0, 0.0).astype(F32)
        for dr in range(nr):
            @pl.when(r == dr)
            def _(dr=dr):
                from_first(stacks[dr])
                from_second(stacks[(dr - plan.hr) % nr])

        factor_rows(w, PANEL)
        inv = w[:, PANEL:]
        inv_hi = inv.astype(BF16)
        inv_out[0] = inv_hi
        inv_out[1] = (inv - inv_hi.astype(F32)).astype(BF16)


def solve_kernel(plan, blocks, live, finish, inv, *rest):
    nr, nc, rb, hr, cw = plan.nr, plan.nc, plan.rb, plan.hr, plan.cw
    fts, pans = rest[:nc], rest[nc:2 * nc]
    ft_relay, rp, cpt, at, kf = rest[2 * nc:]
    r, z = lax.axis_index("row"), lax.axis_index("col")
    nb = rb * nr

    @pl.when(r >= z)
    def _():
        for child in range(plan.children):
            plan.fill(kf, blocks, child)

        def put_front(dz, chunk):
            src = (z + nc - dz) % nc
            at[pl.ds(pl.multiple_of(src * cw, cw), cw), :] = chunk.astype(F32)

        def put_pan(dz, slot):
            piece_id = finish[(z + nc - dz) % nc]
            c, h = piece_id // 2, piece_id % 2
            for which in range(2):
                qb = which * plan.cb
                fb = blocks[c, qb]
                use = fb < PB
                if which:
                    use = use & (h == 1) & (qb < live[c])

                @pl.when(use)
                def _(which=which, fb=fb, c=c, h=h):
                    for s in range(plan.pan):
                        oi, rank = s // plan.rk, s % plan.rk
                        o = h * hr + oi
                        k = plan.first(kf, c, o, r) + rank
                        qa = jnp.minimum(o * rb + k, nb - 1)

                        @pl.when((k < plan.first(kf, c, o, r + 1)) & (qa < live[c]))
                        def _():
                            gi = blocks[c, qa] % plan.group
                            rs = pl.ds(pl.multiple_of(fb * BLK, BLK), BLK)
                            cs = pl.ds(pl.multiple_of(gi * BLK, BLK), BLK)
                            at[rs, cs] = at[rs, cs] + slot(which * plan.pan + s).astype(F32)

        relayed = range(1, nc - 1)
        for dz in range(nc):
            if dz in relayed:
                top = (nc - dz - 2) * cw

                @pl.when(z == 0)
                def _(dz=dz, top=top):
                    put_front(dz, ft_relay[top:top + cw, :])

                @pl.when(z != 0)
                def _(dz=dz):
                    put_front(dz, fts[dz][...])
            else:
                put_front(dz, fts[dz][...])
        for dz in range(nc):
            put_pan(dz, lambda n, dz=dz: pans[dz][n])

        inv_hi, inv_lo = inv[0], inv[1]

        def solve(i, carry):
            cs = pl.ds(pl.multiple_of(i * 256, 256), 256)
            a = at[:, cs]
            a_hi = a.astype(BF16)
            a_lo = (a - a_hi.astype(F32)).astype(BF16)
            p = jnp.dot(inv_hi, a_hi, preferred_element_type=F32)
            p = p + jnp.dot(inv_hi, a_lo, preferred_element_type=F32)
            p = p + jnp.dot(inv_lo, a_hi, preferred_element_type=F32)
            cpt[:, cs] = p.astype(BF16)
            rp[cs, :] = (-jnp.transpose(p)).astype(BF16)
            return carry

        lax.fori_loop(0, plan.local // 256, solve, 0)


def assemble_kernel(plan, blocks, live, finish, *rest):
    nr, nc, rb = plan.nr, plan.nc, plan.rb
    flows = nr * nc
    bulk = rest[:flows]
    acc, kf = rest[flows:]
    r, z = lax.axis_index("row"), lax.axis_index("col")
    nb = rb * nr

    @pl.when(r >= z)
    def _():
        for child in range(plan.children):
            plan.fill(kf, blocks, child)

        def clear(i, carry):
            acc[pl.ds(pl.multiple_of(i * 128, 128), 128), :] = jnp.zeros((128, plan.local), F32)
            return carry

        lax.fori_loop(0, plan.local // 128, clear, 0)

        for k in range(flows):
            src_r = (r + nr - k // nc) % nr
            src_z = (z + nc - k % nc) % nc
            piece_id = finish[src_z]
            c, h = piece_id // 2, piece_id % 2

            def place(s):
                o, flip, rank_a, rank_b, ok = plan.decode(s, src_r, h)
                o = jnp.minimum(o, nr - 1)
                ra = jnp.where(flip, o, src_r)
                rb_ = jnp.where(flip, src_r, o)
                ka = plan.first(kf, c, ra, r) + rank_a
                kb = plan.first(kf, c, rb_, z) + rank_b
                ok = ok & (ka < plan.first(kf, c, ra, r + 1)) & (kb < plan.first(kf, c, rb_, z + 1))
                qa = ra * rb + ka
                qb = rb_ * rb + kb
                pa = ka * nr + plan.res(ra)
                pb = kb * nr + plan.res(rb_)
                ok = ok & (pa >= pb) & (qa >= qb) & (qa < live[c])
                gi = blocks[c, jnp.clip(qa, 0, nb - 1)] % plan.group
                gj = blocks[c, jnp.clip(qb, 0, nb - 1)] % plan.group
                rs = pl.ds(pl.multiple_of(gi * BLK, BLK), BLK)
                cs = pl.ds(pl.multiple_of(gj * BLK, BLK), BLK)
                return ok, flip, rs, cs

            first = plan.rk * plan.rk
            for group in (range(first), range(first, plan.slots)):
                spots = [place(s) for s in group]
                if not spots:
                    continue
                flip = spots[0][1]
                if group.start and plan.hr > 2:
                    parts = [[n] for n in range(len(spots))]
                else:
                    parts = [list(range(len(spots)))]
                for part in parts:
                    flip = spots[part[0]][1]
                    some = spots[part[0]][0]
                    for n in part[1:]:
                        some = some | spots[n][0]

                    @pl.when(some & jnp.logical_not(flip))
                    def _():
                        for n in part:
                            ok, _, rs, cs = spots[n]
                            x = bulk[k][group.start + n].astype(F32)
                            acc[rs, cs] = acc[rs, cs] + jnp.where(ok, x, 0.0)

                    @pl.when(some & flip)
                    def _():
                        turned = [jnp.transpose(bulk[k][group.start + n].astype(F32)) for n in part]
                        for x, n in zip(turned, part):
                            ok, _, rs, cs = spots[n]
                            acc[rs, cs] = acc[rs, cs] + jnp.where(ok, x, 0.0)


def final_kernel(plan, rp, *rest):
    hr = plan.hr
    cpts, acc = rest[:hr], rest[hr]
    out, rpv, cpv, stage, in_sems, out_sems = rest[hr + 1:]
    r, z = lax.axis_index("row"), lax.axis_index("col")
    strip = 256
    strips = plan.local // strip

    def out_copy(i, slot):
        rows = pl.ds(pl.multiple_of(i * strip, strip), strip)
        return pltpu.make_async_copy(stage.at[slot], out.at[rows, :], out_sems.at[slot])

    @pl.when(r < z)
    def _():
        stage[0] = jnp.zeros_like(stage[0])
        stage[1] = jnp.zeros_like(stage[1])

        def body(i, carry):
            @pl.when(i >= 2)
            def _():
                out_copy(i, i % 2).wait()

            out_copy(i, i % 2).start()
            return carry

        lax.fori_loop(0, strips, body, 0)
        out_copy(0, 0).wait()
        out_copy(1, 1).wait()

    @pl.when(r >= z)
    def _():
        rp_copy = pltpu.make_async_copy(rp, rpv, in_sems.at[0])
        rp_copy.start()
        holder = jnp.where((r >= hr) & (z < hr), z + hr, z)
        for d in range(hr):
            @pl.when((r - holder + hr) % hr == d)
            def _(d=d):
                pltpu.make_async_copy(cpts[d], cpv, in_sems.at[1]).start()

        rp_copy.wait()
        pltpu.make_async_copy(cpts[0], cpv, in_sems.at[1]).wait()
        masked = (r == z) | (z == 0)

        def value(i):
            rows = pl.ds(pl.multiple_of(i * strip, strip), strip)
            update = jnp.dot(rpv[rows, :], cpv[...], preferred_element_type=F32)
            return acc[rows, :] + update

        def finish_strip(i, carry):
            slot = i % 2

            @pl.when(i >= 2)
            def _():
                out_copy(i, slot).wait()

            @pl.when(masked)
            def _():
                row_ids = r * plan.local + i * strip + lax.broadcasted_iota(jnp.int32, (strip, plan.local), 0)
                col_ids = z * plan.local + lax.broadcasted_iota(jnp.int32, (strip, plan.local), 1)
                keep = (row_ids >= col_ids) & (col_ids >= PANEL)
                stage[slot] = jnp.where(keep, value(i), 0.0).astype(BF16)

            @pl.when(jnp.logical_not(masked))
            def _():
                stage[slot] = value(i).astype(BF16)

            out_copy(i, slot).start()
            return carry

        lax.fori_loop(0, strips, finish_strip, 0)
        out_copy(0, 0).wait()
        out_copy(1, 1).wait()


def body(front_cols, contrib, child_blocks, child_live, finish):
    nr, nc = lax.axis_size("row"), lax.axis_size("col")
    own_row, own_col = lax.axis_index("row"), lax.axis_index("col")
    local = front_cols.shape[0]
    children = child_blocks.shape[0]
    plan = Plan(nr, nc, local, contrib.shape[1], contrib.shape[2], children)
    flows = nr * nc
    both = ("row", "col")

    def pairs(dr, dz, wanted):
        found = []
        for r in range(nr):
            for z in range(nc):
                to_r, to_c = (r + dr) % nr, (z + dz) % nc
                if wanted(r, z, to_r, to_c):
                    found.append((r * nc + z, to_r * nc + to_c))
        return found

    def send(x, dr, dz, wanted):
        return lax.ppermute(x, both, pairs(dr, dz, wanted))

    def in_vmem(x):
        return pltpu.with_memory_space_constraint(x, pltpu.VMEM)

    smem = pl.BlockSpec(memory_space=pltpu.SMEM)
    vmem = pl.BlockSpec(memory_space=pltpu.VMEM)
    anyw = pl.BlockSpec(memory_space=pl.ANY)
    slot_shape = (plan.slots, BLK, BLK)

    source_row = lambda r, z, R, C: r % plan.hr == 0
    lower = lambda r, z, R, C: R >= C

    ft = front_cols.T
    packed = pl.pallas_call(
        functools.partial(pack_kernel, plan),
        name="pack",
        in_specs=[smem, smem, vmem, vmem],
        out_specs=[vmem] * (flows + nr + 1),
        out_shape=[pltpu.HBM(slot_shape, BF16)] * flows
        + [jax.ShapeDtypeStruct((plan.pan, BLK, BLK), BF16)] * nr
        + [jax.ShapeDtypeStruct((BLK + PB * plan.cw, BLK), BF16)],
        scratch_shapes=[plan.table()],
        compiler_params=pltpu.CompilerParams(vmem_limit_bytes=24 << 20),
    )(child_blocks, finish, contrib, ft)
    bulk, pan, corner = packed[:flows], packed[flows:-1], packed[-1]
    corners = [corner] + [send(corner, 0, dz, source_row) for dz in range(1, nc)]

    direct = lambda r, z, R, C: (R >= C or C == 1) and (C > 0 or z < 2)
    last_hop = lambda r, z, R, C: z == 1
    passed_on = [(1 - z) % nc for z in range(2, nc)]
    fts = [ft] + [send(ft, 0, dz, direct) for dz in range(1, nc)]
    ft_relay = send(jnp.concatenate([fts[dz] for dz in passed_on]), 0, nc - 1, last_hop)

    corners = jnp.concatenate(corners)
    stacks = [corners] + [send(corners, dr, 0, source_row) for dr in range(1, nr)]
    pans = [pan[0]] + [send(pan[dr], dr, 0, source_row) for dr in range(1, nr)]

    def from_row(row):
        shift = (own_row - row) % nr
        got = pans[0]
        for dr in range(1, nr):
            got = jnp.where(shift == dr, pans[dr], got)
        return got

    pan_own = jnp.concatenate([from_row(0), from_row(plan.hr)])
    pan_all = [pan_own] + [send(pan_own, 0, dz, lower) for dz in range(1, nc)]
    received = [bulk[0]] + [send(bulk[k], k // nc, k % nc, lower) for k in range(1, flows)]

    inv = pl.pallas_call(
        functools.partial(factor_kernel, plan),
        name="factor",
        in_specs=[smem] * 3 + [vmem] * nr,
        out_specs=vmem,
        out_shape=jax.ShapeDtypeStruct((2, PANEL, PANEL), BF16),
        scratch_shapes=[pltpu.VMEM((PANEL, 2 * PANEL), F32)],
        compiler_params=pltpu.CompilerParams(vmem_limit_bytes=12 << 20),
    )(child_blocks, child_live, finish, *[in_vmem(x) for x in stacks])

    rp, cpt = pl.pallas_call(
        functools.partial(solve_kernel, plan),
        name="solve",
        in_specs=[smem] * 3 + [vmem] * (2 + 2 * nc),
        out_specs=[vmem, vmem],
        out_shape=[jax.ShapeDtypeStruct((local, PANEL), BF16), jax.ShapeDtypeStruct((PANEL, local), BF16)],
        scratch_shapes=[pltpu.VMEM((PANEL, local), F32), plan.table()],
        compiler_params=pltpu.CompilerParams(vmem_limit_bytes=24 << 20),
    )(child_blocks, child_live, finish, inv, *fts, *pan_all, ft_relay)

    across = send(cpt, plan.hr, 0, lambda r, z, R, C: r == z and R > r)
    held = jnp.where(own_row == own_col, cpt, across)
    cpts = [held]
    for d in range(1, plan.hr):
        found = []
        for r in range(nr):
            base = r // plan.hr * plan.hr
            to_r = base + (r - base + d) % plan.hr
            for z in range(nc):
                if (r == z and to_r > r) or r == z + plan.hr:
                    found.append((r * nc + z, to_r * nc + z))
        cpts.append(lax.ppermute(held, both, found))

    acc = pl.pallas_call(
        functools.partial(assemble_kernel, plan),
        name="assemble",
        in_specs=[smem] * 3 + [vmem] * flows,
        out_specs=vmem,
        out_shape=pltpu.VMEM((local, local), F32),
        scratch_shapes=[plan.table()],
        compiler_params=pltpu.CompilerParams(vmem_limit_bytes=8 << 20),
    )(child_blocks, child_live, finish, *[in_vmem(x) for x in received])

    return pl.pallas_call(
        functools.partial(final_kernel, plan),
        name="final",
        in_specs=[anyw] * (1 + plan.hr) + [vmem],
        out_specs=anyw,
        out_shape=jax.ShapeDtypeStruct((local, local), BF16),
        scratch_shapes=[
            pltpu.VMEM((local, PANEL), BF16),
            pltpu.VMEM((PANEL, local), BF16),
            pltpu.VMEM((2, 256, local), BF16),
            pltpu.SemaphoreType.DMA((2,)),
            pltpu.SemaphoreType.DMA((2,)),
        ],
        compiler_params=pltpu.CompilerParams(vmem_limit_bytes=20 << 20),
    )(rp, *cpts, acc)


def solution(mesh):
    return jax.shard_map(
        body,
        mesh=mesh,
        in_specs=(
            P(("front", "row"), "col"),
            P(("front", "col"), "row", None),
            P("front", None),
            P("front"),
            P("front"),
        ),
        out_specs=P(("front", "row"), "col"),
        check_vma=False,
    )
```
